1024 devices in a mesh: ep: 16 (over y_hi, x), edp: 16 (over z), tp: 4 (over y_lo, core).
Axes of the slice: x: 4, y: 8 (y_hi: 4, y_lo: 2; y = y_hi * 2 + y_lo), z: 16, core: 2. Of those that a mesh axis runs over, the one named last changes fastest.
Arguments:
- tokens: bfloat16 [32768, 4096], P(('ep', 'edp'), 'tp'), may hold values from -6 to 6
- cotangent: bfloat16 [32768, 4096], P(('ep', 'edp'), 'tp'), may hold values from -6 to 6
- expert_ids: int32 [32768, 8], P(('ep', 'edp')), may hold values from 0 to 127, all different within a row; in each aligned block of 128 rows (0 to 127, 128 to 255, ...) at most 10 rows name the same one
- route_weights: float32 [32768, 8], P(('ep', 'edp')), may hold values from 0.1 to 1
- expert_weights: bfloat16 [3, 6144, 4096], P(None, ('ep', 'tp')), may hold values from -0.15625 to 0.15625
Outputs:
- mixed: bfloat16 [32768, 4096], P(('ep', 'edp'), 'tp')
- grad_tokens: bfloat16 [32768, 4096], P(('ep', 'edp'), 'tp')
- weight_grads: float32 [3, 6144, 4096], P(None, ('ep', 'tp'), 'edp')
The draws below stay inside these ranges and needn't reach their ends.
Inputs may be any that keep to these rules, and one draw needn't show every extreme that they name: `expert_ids`: each token names 8 different experts; within the tokens of one (ep, edp) index no expert is named by more than 10 tokens.
All inputs are finite; a program needn't handle non-finite values.
Results may differ from the reference program's by a relative error of at most 0.017.
Values may be sent and summed in bfloat16 or wider, within the bound.
No kernel may reach another device: no remote copies, remote signals or barrier semaphores. Data moves between devices by JAX's collectives and lax.ppermute only.
A program may use at most 64 MiB of HBM per device.

```python
import math
import jax
import jax.numpy as jnp
import numpy as np
from jax import lax

D = 4096
FF = 1536
EXPERTS = 128
TOP = 8
TOK_DEV = 128
CAP = 10
EXP_WIN = 4
SLICE = 96
TOKENS = 32768
N_EP = 16
N_EDP = 16
N_TP = 4


def block_levels(key, extent, shards, least, high):
    factor_of = 1.0
    for axis_at, blocks in shards:
        heights = jax.random.uniform(jax.random.fold_in(jax.random.fold_in(key, 6), axis_at), (blocks,), jnp.float32, least / len(shards), high / len(shards))
        factor_of = factor_of * jnp.repeat(jnp.exp(heights), extent[axis_at] // blocks).reshape((-1,) + (1,) * (len(extent) - 1 - axis_at))
    return factor_of


def deal_out(rng, own, number, rows, count, top, limit, slope):
    sequence = jax.random.permutation(rng, count)
    heavy_load, common = load_shares(count, rows * top, limit, slope, True), load_shares(count, rows * top, limit, slope, False)
    places = jnp.arange(count)

    def named(sizes, turn):
        used = int((sizes > 0).sum())
        fixed = max(1, used // 4)
        passed = fixed + (places - fixed + turn * (used - fixed)) % max(1, count - fixed)
        return jnp.zeros((count,), jnp.int32).at[sequence[jnp.where(places < fixed, places, passed)]].set(jnp.asarray(sizes, jnp.int32))

    sizes = jnp.where(number % 4 == 0, named(heavy_load, number // 4), named(common, number - number // 4 - 1))
    mixed = jax.random.permutation(jax.random.fold_in(own, 3), count)
    donor, taker = mixed[0:count // 2 * 2:2], mixed[1:count // 2 * 2:2]
    margin = jnp.minimum(sizes[donor] - 1, limit - sizes[taker]) // 2
    margin = jnp.where((donor == sequence[0]) | (taker == sequence[0]) | (sizes[taker] == 0), 0, jnp.maximum(margin, 0))
    passed = jax.random.randint(jax.random.fold_in(own, 4), (count // 2,), 0, 1 << 20) % (margin + 1)
    sizes = sizes.at[donor].add(-passed).at[taker].add(passed)
    labels = jnp.searchsorted(jnp.cumsum(sizes), jnp.arange(rows * top), side="right").astype(jnp.int32)
    listing = labels.reshape(top, rows).T
    listing = listing[jax.random.permutation(jax.random.fold_in(own, 1), rows)]
    turn = jax.random.randint(jax.random.fold_in(own, 2), (rows, 1), 0, top)
    return jnp.take_along_axis(listing, (jnp.arange(top)[None, :] + turn) % top, axis=1)


def load_shares(count, total, bound, lean, full):
    loads = [(1 << 20) // math.isqrt(standing ** lean) + 1 for standing in range(1, count + 1)]
    largest = bound if full else min(bound, max(-(-total // count), total * loads[0] // sum(loads)))
    least = 1 if total - largest >= count - 1 else 0
    counts, surplus = [largest] + [least] * (count - 1), total - largest - least * (count - 1)
    while surplus > 0:
        movable = [i for i in range(1, count) if counts[i] < largest] or [i for i in range(1, count) if counts[i] < bound]
        pool, remaining = sum([loads[i] for i in movable]), surplus
        for i in movable:
            addition = min(bound - counts[i], max(1, remaining * loads[i] // pool), surplus)
            counts[i] = counts[i] + addition
            surplus = surplus - addition
    return np.array(counts)


def noise(rng, shape, width, most, cuts=(), held_as=jnp.bfloat16):
    loudness = block_levels(rng, shape, cuts, -0.22, 0.18) if cuts else 1.0
    result = jax.random.normal(rng, shape, jnp.float32) * width * loudness
    return jnp.minimum(jnp.maximum(result, -most), most).astype(held_as)


def setup_inputs(seed: int = 0) -> dict:
    splits = jax.random.split(jax.random.key(seed), 6)
    tokens = noise(splits[0], (TOKENS, D), 1.0, 6.0, ((0, 256), (1, 4)))
    cotangent = noise(splits[1], (TOKENS, D), 1.0, 6.0, ((0, 256), (1, 4)))
    expert_ids_keys = jax.random.split(jax.random.fold_in(splits[2], 1), TOKENS // TOK_DEV)
    expert_ids_turns = jax.random.permutation(jax.random.fold_in(splits[2], 3), TOKENS // TOK_DEV)
    expert_ids = jax.vmap(lambda own, number: deal_out(jax.random.fold_in(splits[2], 2), own, number, TOK_DEV, EXPERTS, TOP, CAP, 1))(expert_ids_keys, expert_ids_turns).reshape((TOKENS, TOP))
    route_weights = jnp.clip(jnp.exp(math.log(1.0) - 2.3025851 * jax.random.uniform(splits[3], (TOKENS, TOP), jnp.float32) ** block_levels(splits[3], (TOKENS, TOP), ((0, 256),), -0.2, 0.2)), 0.1, 1.0)
    expert_weights = noise(splits[4], (3, EXP_WIN * FF, D), FF ** -0.5, 0.15625, ((1, 64),))
    return {"tokens": tokens, "cotangent": cotangent, "expert_ids": expert_ids, "route_weights": route_weights, "expert_weights": expert_weights}


def settle(values):
    return lax.optimization_barrier(values.astype(jnp.bfloat16)).astype(jnp.float32)


def reference(tokens, cotangent, expert_ids, route_weights, expert_weights):
    groups = N_EP * N_EDP
    window = N_EP // 4
    per_group = TOK_DEV * TOP
    flat_ids = expert_ids.reshape(groups, per_group)
    matches = (flat_ids[:, :, None] == jnp.arange(window, dtype=jnp.int32)[None, None, :]).astype(jnp.int32)
    slot_index = jnp.sum(matches * (jnp.cumsum(matches, axis=1) - 1), axis=2).astype(jnp.int32)
    owner = jnp.where(jnp.sum(matches, axis=2) > 0, flat_ids, window).astype(jnp.int32)
    token_index = (jnp.arange(groups, dtype=jnp.int32)[:, None] * TOK_DEV
                   + jnp.arange(per_group, dtype=jnp.int32)[None, :] // TOP).astype(jnp.int32)
    group_index = jnp.broadcast_to(jnp.arange(groups, dtype=jnp.int32)[:, None], flat_ids.shape).astype(jnp.int32)
    slot_token = jnp.zeros((window, groups, CAP), jnp.int32).at[owner, group_index, slot_index].set(token_index, mode="drop")
    slot_weight = jnp.zeros((window, groups, CAP), jnp.float32).at[owner, group_index, slot_index].set(
        route_weights.reshape(groups, per_group), mode="drop")
    slot_live = jnp.zeros((window, groups, CAP), jnp.float32).at[owner, group_index, slot_index].set(
        jnp.ones((groups, per_group), jnp.float32), mode="drop")
    expert_blocks = jnp.moveaxis(expert_weights.reshape(3, window, 4, N_TP, SLICE, D), 1, 0)
    row_count = groups * CAP

    def one_expert(operands):
        slot_toks, slot_wts, slot_flags, blocks = operands
        flat_tok = slot_toks.reshape(-1)
        live_col = slot_flags.reshape(-1, 1)
        rows = tokens[flat_tok] * live_col.astype(jnp.bfloat16)
        scaled = (cotangent[flat_tok].astype(jnp.float32) * (slot_wts.reshape(-1, 1) * live_col)).astype(jnp.bfloat16)
        rows_wide = rows.astype(jnp.float32).reshape(N_EP, N_EDP, CAP, D)
        scaled_wide = scaled.astype(jnp.float32).reshape(N_EP, N_EDP, CAP, D)

        def per_replica(left, right_wide):
            left_wide = left.astype(jnp.float32).reshape(N_EP, N_EDP, CAP, SLICE)
            partial_sums = jnp.einsum("pics,picd->isd", left_wide, right_wide, precision=lax.Precision.HIGHEST)
            return jnp.sum(settle(partial_sums), axis=0)

        def one_slice(carry, slab):
            out_acc, back_acc = carry
            gate_w, up_w, down_w = slab[0], slab[1], slab[2]
            gate_val = jnp.dot(rows, gate_w.T, preferred_element_type=jnp.float32)
            up_val = jnp.dot(rows, up_w.T, preferred_element_type=jnp.float32)
            sigmoid_gate = jax.nn.sigmoid(gate_val)
            active = gate_val * sigmoid_gate
            hidden = (active * up_val).astype(jnp.bfloat16)
            out_part = jnp.dot(hidden, down_w, preferred_element_type=jnp.float32)
            d_hidden = jnp.dot(scaled, down_w.T, preferred_element_type=jnp.float32)
            d_gate = (d_hidden * up_val * sigmoid_gate * (1.0 + gate_val * (1.0 - sigmoid_gate))).astype(jnp.bfloat16)
            d_up = (d_hidden * active).astype(jnp.bfloat16)
            back_part = (jnp.dot(d_gate, gate_w, preferred_element_type=jnp.float32)
                         + jnp.dot(d_up, up_w, preferred_element_type=jnp.float32))
            grad_slab = jnp.stack([per_replica(d_gate, rows_wide), per_replica(d_up, rows_wide),
                                   per_replica(hidden, scaled_wide)])
            return (out_acc + settle(out_part), back_acc + settle(back_part)), grad_slab

        out_total = jnp.zeros((row_count, D), jnp.float32)
        back_total = jnp.zeros((row_count, D), jnp.float32)
        grad_list = []
        for half_index in range(4):
            start = (jnp.zeros((row_count, D), jnp.float32), jnp.zeros((row_count, D), jnp.float32))
            slabs = jnp.moveaxis(blocks[:, half_index], 1, 0)
            (out_half, back_half), grad_half = lax.scan(one_slice, start, slabs)
            out_total = out_total + settle(out_half)
            back_total = back_total + settle(back_half)
            grad_list.append(grad_half)
        return out_total, back_total, jnp.stack(grad_list)

    outs, backs, grads = lax.map(one_expert, (slot_token, slot_weight, slot_live, expert_blocks))
    weight_grads = jnp.moveaxis(grads, 3, 0).reshape(3, window * FF, D)
    flat_tok = slot_token.reshape(-1)
    mixed = jnp.zeros((groups * TOK_DEV, D), jnp.float32).at[flat_tok].add(
        (slot_weight * slot_live).reshape(-1, 1) * outs.reshape(-1, D)).astype(jnp.bfloat16)
    grad_tokens = jnp.zeros((groups * TOK_DEV, D), jnp.float32).at[flat_tok].add(
        slot_live.reshape(-1, 1) * backs.reshape(-1, D)).astype(jnp.bfloat16)
    return mixed, grad_tokens, weight_grads
```

```python
import functools

import jax
import jax.numpy as jnp
from jax import lax
from jax.experimental import pallas as pl
from jax.experimental.pallas import tpu as pltpu
from jax.sharding import Mesh, PartitionSpec as P

HALF = 12
BLOCK = 2 * HALF
F32, BF16 = jnp.float32, jnp.bfloat16
VMEM = pl.BlockSpec(memory_space=pltpu.VMEM)
SMEM = pl.BlockSpec(memory_space=pltpu.SMEM)


def dot(a, b, contract, **kw):
    return lax.dot_general(a, b, ((contract[:1], contract[1:]), ((), ())), preferred_element_type=F32, **kw)


def pack_kernel(copies, ids_ref, wts_ref, tok_ref, cot_ref, out_ref, sel_ref, selw_ref):
    window = out_ref.shape[0]
    n_tok = tok_ref.shape[0]
    ids = ids_ref[...]
    wts = wts_ref[...]
    rows = [jnp.max((ids == e).astype(F32), axis=0, keepdims=True) for e in range(window)]
    named = jnp.concatenate(rows + [jnp.zeros((8 - window, n_tok), F32)], axis=0)
    before = lax.broadcasted_iota(jnp.int32, (n_tok, n_tok), 0) < lax.broadcasted_iota(jnp.int32, (n_tok, n_tok), 1)
    rank = dot(named.astype(BF16), before.astype(BF16), (1, 0)).astype(jnp.int32)
    row = lax.broadcasted_iota(jnp.int32, (BLOCK, n_tok), 0)
    slot = jnp.where(row < HALF, row, row - HALF)
    tok = tok_ref[...]
    cot = cot_ref[...]
    for e in range(window):
        hit = jnp.logical_and(slot == rank[e : e + 1], named[e : e + 1] > 0.5)
        weight = jnp.sum(jnp.where(ids == e, wts, 0.0), axis=0, keepdims=True)
        pick_tok = jnp.where(jnp.logical_and(hit, row < HALF), 1.0, 0.0)
        pick_cot = jnp.where(jnp.logical_and(hit, row >= HALF), 1.0, 0.0)
        selw = pick_cot * weight
        scale = jnp.where(row[:, :1] < HALF, 1.0, jnp.sum(selw, axis=1, keepdims=True))
        picked = dot(pick_tok.astype(BF16), tok, (1, 0)) + dot(pick_cot.astype(BF16), cot, (1, 0))
        block = (picked * scale).astype(BF16)
        for k in range(copies):
            out_ref[e, k] = block
        sel_ref[e * BLOCK : (e + 1) * BLOCK] = pick_tok
        selw_ref[e * BLOCK : (e + 1) * BLOCK] = selw


def expert_kernel(core_ref, own_ref, other_ref, w_ref, y_own_ref, y_other_ref, g_ref):
    core = core_ref[0]
    n_src, n_yl, _, width = own_ref.shape
    n_rows = n_src * BLOCK
    hid = w_ref.shape[1]
    blocks = []
    for yl in range(n_yl):
        blocks.append((own_ref, y_own_ref, yl, 2 * yl + core))
        blocks.append((other_ref, y_other_ref, yl, 2 * yl + 1 - core))

    def weights(t):
        cols = pl.ds(pl.multiple_of(t * width, width), width)
        return w_ref[:, :, cols].reshape(3 * hid, width)

    proj = jnp.zeros((3 * hid, n_rows), F32)
    for x_ref, _, yl, t in blocks:
        proj = proj + dot(weights(t), x_ref[:, yl].reshape(n_rows, width), (1, 1))
    lane = lax.broadcasted_iota(jnp.int32, (hid, n_rows), 1)
    live = lax.rem(lane, BLOCK) < HALF
    gate = proj[:hid]
    up = proj[hid : 2 * hid]
    d_hidden = pltpu.roll(proj[2 * hid :], n_rows - HALF, 1)
    sig = jax.nn.sigmoid(gate)
    active = gate * sig
    hidden = jnp.where(live, active * up, 0.0)
    d_gate = jnp.where(live, d_hidden * up * sig * (1.0 + gate * (1.0 - sig)), 0.0)
    d_up = jnp.where(live, d_hidden * active, 0.0)
    left = jnp.concatenate([d_gate, d_up, pltpu.roll(hidden, HALF, 1)], axis=0)
    left_t = left.T.astype(BF16)
    left = left.astype(BF16)
    for x_ref, y_ref, yl, t in blocks:
        cols = pl.ds(pl.multiple_of(t * width, width), width)
        grad = dot(left, x_ref[:, yl].reshape(n_rows, width), (1, 0))
        g_ref[:, :, cols] = grad.astype(BF16).reshape(3, hid, width)
        y = dot(left_t, weights(t), (1, 0))
        y_ref[:, yl] = y.astype(BF16).reshape(n_src, BLOCK, width)


def combine_kernel(z_ref, sel_ref, selw_ref, mixed_ref, grad_ref):
    window, copies = z_ref.shape[:2]
    total = z_ref[:, 0].astype(F32)
    for k in range(1, copies):
        total = total + z_ref[:, k].astype(F32)
    total = total.reshape(window * BLOCK, z_ref.shape[3])
    exact = dict(precision=lax.Precision.HIGHEST)
    mixed_ref[...] = dot(selw_ref[...], total, (0, 0), **exact).astype(BF16)
    grad_ref[...] = dot(sel_ref[...], total, (0, 0), **exact).astype(BF16)


def call(kernel, out_shapes, args, smem=0):
    return pl.pallas_call(
        kernel,
        out_shape=[jax.ShapeDtypeStruct(s, d) for s, d in out_shapes],
        in_specs=[SMEM] * smem + [VMEM] * (len(args) - smem),
        out_specs=[VMEM] * len(out_shapes),
        compiler_params=pltpu.CompilerParams(vmem_limit_bytes=48 * 1024 * 1024),
    )(*args)


def shards(tokens, cotangent, expert_ids, route_weights, expert_weights):
    n_yh, n_x, n_yl = (lax.axis_size(a) for a in ("yh", "x", "yl"))
    window = n_yh
    n_tok, width = tokens.shape
    plane = ("yh", "x", "yl")
    copies = n_x * n_yl
    n_src = n_yh * n_x
    swap = [(0, 1), (1, 0)]

    packed, sel, selw = call(
        functools.partial(pack_kernel, copies),
        [((window, copies, BLOCK, width), BF16)] + [((window * BLOCK, n_tok), F32)] * 2,
        (expert_ids.T, route_weights.T, tokens, cotangent),
    )
    own = lax.all_to_all(packed.reshape(-1, BLOCK, width), plane, 0, 0, tiled=True)
    other = lax.ppermute(own, "c", swap)
    shape = (n_src, n_yl, BLOCK, width)
    core = lax.axis_index("c").astype(jnp.int32).reshape(1)
    y_own, y_other, grads = call(
        expert_kernel,
        [(shape, BF16), (shape, BF16), (expert_weights.shape, BF16)],
        (core, own.reshape(shape), other.reshape(shape), expert_weights),
        smem=1,
    )
    weight_grads = lax.psum_scatter(grads, "z", scatter_dimension=2, tiled=True).astype(F32)
    partner = lax.ppermute(y_other, "c", swap)
    y = (y_own.astype(F32) + partner.astype(F32)).astype(BF16)
    home = lax.all_to_all(y.reshape(-1, BLOCK, width), plane, 0, 0, tiled=True)
    mixed, grad_tokens = call(
        combine_kernel,
        [((n_tok, width), BF16)] * 2,
        (home.reshape(window, copies, BLOCK, width), sel, selw),
    )
    return mixed, grad_tokens, weight_grads


def solution(mesh):
    n_ep, n_edp, n_tp = mesh.devices.shape
    side = 4
    fine = Mesh(
        mesh.devices.reshape(side, n_ep // side, n_edp, n_tp // 2, 2), ("yh", "x", "z", "yl", "c")
    )
    group, feat = ("yh", "x", "z"), ("yl", "c")
    hid = ("yh", "x", "yl", "c")
    placed = (P(group, feat), P(group, feat), P(group, None), P(group, None), P(None, hid, None))
    return jax.shard_map(
        shards,
        mesh=fine,
        in_specs=placed,
        out_specs=(P(group, feat), P(group, feat), P(None, hid, "z")),
        check_vma=False,
    )
```

```python
import functools

import jax
import jax.numpy as jnp
from jax import lax
from jax.experimental import pallas as pl
from jax.experimental.pallas import tpu as pltpu
from jax.sharding import Mesh, PartitionSpec as P


HALF = 12
BLOCK = 2 * HALF
F32, BF16 = jnp.float32, jnp.bfloat16
VMEM = pl.BlockSpec(memory_space=pltpu.VMEM)
SMEM = pl.BlockSpec(memory_space=pltpu.SMEM)
HBM = pl.BlockSpec(memory_space=pltpu.HBM)


def dot(a, b, contract, **kw):
    return lax.dot_general(a, b, ((contract[:1], contract[1:]), ((), ())), preferred_element_type=F32, **kw)


def pack_kernel(copies, ids_hbm, wts_hbm, tok_hbm, cot_hbm, out_ref, sel_ref, selw_ref, ids_ref, wts_ref, tok_ref, cot_ref, sems):
    pairs = ((ids_hbm, ids_ref), (wts_hbm, wts_ref), (tok_hbm, tok_ref), (cot_hbm, cot_ref))
    moves = [pltpu.make_async_copy(src, dst, sems.at[k]) for k, (src, dst) in enumerate(pairs)]
    for move in moves:
        move.start()
    window = out_ref.shape[0]
    n_tok = tok_ref.shape[0]
    before = lax.broadcasted_iota(jnp.int32, (n_tok, n_tok), 0) < lax.broadcasted_iota(jnp.int32, (n_tok, n_tok), 1)
    row = lax.broadcasted_iota(jnp.int32, (BLOCK, n_tok), 0)
    slot = jnp.where(row < HALF, row, row - HALF)
    moves[0].wait()
    moves[1].wait()
    ids = ids_ref[...]
    wts = wts_ref[...]
    rows = [jnp.max((ids == e).astype(F32), axis=0, keepdims=True) for e in range(window)]
    named = jnp.concatenate(rows + [jnp.zeros((8 - window, n_tok), F32)], axis=0)
    rank = dot(named.astype(BF16), before.astype(BF16), (1, 0)).astype(jnp.int32)
    moves[2].wait()
    moves[3].wait()
    tok = tok_ref[...]
    cot = cot_ref[...]
    for e in range(window):
        hit = jnp.logical_and(slot == rank[e : e + 1], named[e : e + 1] > 0.5)
        weight = jnp.sum(jnp.where(ids == e, wts, 0.0), axis=0, keepdims=True)
        pick_tok = jnp.where(jnp.logical_and(hit, row < HALF), 1.0, 0.0)
        pick_cot = jnp.where(jnp.logical_and(hit, row >= HALF), 1.0, 0.0)
        selw = pick_cot * weight
        scale = jnp.where(row[:, :1] < HALF, 1.0, jnp.sum(selw, axis=1, keepdims=True))
        picked = dot(pick_tok.astype(BF16), tok, (1, 0)) + dot(pick_cot.astype(BF16), cot, (1, 0))
        block = (picked * scale).astype(BF16)
        for k in range(copies):
            out_ref[e, k] = block
        sel_ref[e * BLOCK : (e + 1) * BLOCK] = pick_tok
        selw_ref[e * BLOCK : (e + 1) * BLOCK] = selw


def feature_blocks(core, n_yl):
    for yl in range(n_yl):
        yield 0, yl, 2 * yl + core
        yield 1, yl, 2 * yl + 1 - core


def columns(t, width):
    return pl.ds(pl.multiple_of(t * width, width), width)


def stacked(refs, yl):
    parts = [r[:, yl] for r in refs]
    return [p.reshape(p.shape[0] * p.shape[1], p.shape[2]) for p in parts]


def project_kernel(n_each, core_ref, *refs):
    sides = refs[:n_each], refs[n_each : 2 * n_each]
    w_ref, p_ref = refs[2 * n_each :]
    width = refs[0].shape[3]
    total = jnp.zeros(p_ref.shape, F32)
    for side, yl, t in feature_blocks(core_ref[0], refs[0].shape[1]):
        w = w_ref[:, :, columns(t, width)].reshape(p_ref.shape[0], width)
        total = total + dot(w, jnp.concatenate(stacked(sides[side], yl), axis=0), (1, 1))
    p_ref[...] = total


def grad_kernel(n_near, n_far, core_ref, p_ref, *refs):
    n_each = n_near + n_far
    sides = refs[:n_each], refs[n_each : 2 * n_each]
    w_ref, g_ref, left_ref, proj_ref = refs[2 * n_each :]
    width = refs[0].shape[3]
    n_yl = refs[0].shape[1]
    rows = proj_ref.shape[0]
    hid = rows // 3
    lanes = proj_ref.shape[1]
    near = p_ref.shape[1]
    far = sum(r.shape[0] for r in refs[n_near:n_each]) * BLOCK
    blocks = list(feature_blocks(core_ref[0], n_yl))
    total = jnp.zeros((rows, far), F32)
    for side, yl, t in blocks:
        w = w_ref[:, :, columns(t, width)].reshape(rows, width)
        total = total + dot(w, jnp.concatenate(stacked(sides[side][n_near:], yl), axis=0), (1, 1))
    proj_ref[...] = jnp.zeros(proj_ref.shape, F32)
    proj_ref[:, :far] = total
    proj_ref[:, 128 : 128 + near] = p_ref[...]
    gate = proj_ref[:hid]
    up = proj_ref[hid : 2 * hid]
    lane = lax.broadcasted_iota(jnp.int32, (hid, lanes), 1)
    place = jnp.where(lane < 128, lane, lane - 128)
    inside = jnp.logical_or(lane < far, jnp.logical_and(lane >= 128, lane < 128 + near))
    live = jnp.logical_and(inside, lax.rem(place, BLOCK) < HALF)
    d_hidden = pltpu.roll(proj_ref[2 * hid :], lanes - HALF, 1)
    sig = jax.nn.sigmoid(gate)
    active = gate * sig
    hidden = jnp.where(live, active * up, 0.0)
    d_gate = jnp.where(live, d_hidden * up * sig * (1.0 + gate * (1.0 - sig)), 0.0)
    d_up = jnp.where(live, d_hidden * active, 0.0)
    left = jnp.concatenate([d_gate, d_up, pltpu.roll(hidden, HALF, 1)], axis=0).astype(BF16)
    left_ref[...] = left
    pad = [jnp.zeros((128 - far, width), BF16)]
    tail = [jnp.zeros((lanes - 128 - near, width), BF16)]
    for side, yl, t in blocks:
        parts = stacked(sides[side], yl)
        x = jnp.concatenate(parts[n_near:] + pad + parts[:n_near] + tail, axis=0)
        g_ref[:, :, columns(t, width)] = dot(left, x, (1, 0)).astype(BF16).reshape(3, hid, width)


def output_kernel(near, far, core_ref, left_ref, w_ref, y_own_ref, y_other_ref):
    core, x = core_ref[0], core_ref[1]
    n_yh, n_x, n_yl, _, width = y_own_ref.shape
    each = n_yh * BLOCK
    left_t = left_ref[...].astype(F32).T.astype(BF16)
    rows = jnp.concatenate([left_t[128 : 128 + near], left_t[:far]], axis=0)
    for side, yl, t in feature_blocks(core, n_yl):
        w = w_ref[:, :, columns(t, width)].reshape(rows.shape[1], width)
        y = dot(rows, w, (1, 0)).astype(BF16)
        y_ref = y_other_ref if side else y_own_ref
        for slot, flip in enumerate((0, 1, 3, 2)):
            y_ref[:, jnp.bitwise_xor(x, flip), yl] = y[slot * each : (slot + 1) * each].reshape(n_yh, BLOCK, width)


def combine_kernel(z_ref, sel_ref, selw_ref, mixed_ref, grad_ref):
    window, copies = z_ref.shape[:2]
    total = z_ref[:, 0].astype(F32)
    for k in range(1, copies):
        total = total + z_ref[:, k].astype(F32)
    total = total.reshape(window * BLOCK, z_ref.shape[3])
    exact = dict(precision=lax.Precision.HIGHEST)
    mixed_ref[...] = dot(selw_ref[...], total, (0, 0), **exact).astype(BF16)
    grad_ref[...] = dot(sel_ref[...], total, (0, 0), **exact).astype(BF16)


def call(kernel, out_shapes, args, smem=0, flops=0, in_space=VMEM, scratch=(), limit=40 * 1024 * 1024):
    return pl.pallas_call(
        kernel,
        out_shape=[jax.ShapeDtypeStruct(s, d) for s, d in out_shapes],
        in_specs=[SMEM] * smem + [in_space] * (len(args) - smem),
        out_specs=[VMEM] * len(out_shapes),
        scratch_shapes=list(scratch),
        cost_estimate=pl.CostEstimate(flops=flops, bytes_accessed=1 << 20, transcendentals=0),
        compiler_params=pltpu.CompilerParams(vmem_limit_bytes=limit),
    )(*args)


def shards(tokens, cotangent, expert_ids, route_weights, expert_weights):
    n_yh, n_x, n_yl = (lax.axis_size(a) for a in ("yh", "x", "yl"))
    window = n_yh
    n_tok, width = tokens.shape
    hid = expert_weights.shape[1]
    swap = [(0, 1), (1, 0)]
    pair_a = [(0, 1), (1, 0), (2, 3), (3, 2)]
    pair_b = [(1, 2), (2, 1), (3, 0), (0, 3)]
    each = n_yh * BLOCK

    packed, sel, selw = call(
        functools.partial(pack_kernel, n_yl),
        [((window, n_yl, BLOCK, width), BF16)] + [((window * BLOCK, n_tok), F32)] * 2,
        (expert_ids.T, route_weights.T, tokens, cotangent),
        in_space=HBM,
        limit=60 * 1024 * 1024,
        scratch=[
            pltpu.VMEM(expert_ids.shape[::-1], jnp.int32),
            pltpu.VMEM(route_weights.shape[::-1], F32),
            pltpu.VMEM(tokens.shape, BF16),
            pltpu.VMEM(cotangent.shape, BF16),
            pltpu.SemaphoreType.DMA((4,)),
        ],
        flops=1 << 26,
    )
    mine = lax.all_to_all(packed.reshape(-1, BLOCK, width), ("yh", "yl"), 0, 0, tiled=True)
    mine = mine.reshape(n_yh, n_yl, BLOCK, width)
    from_a = lax.ppermute(mine, "x", pair_a)
    from_b = lax.ppermute(mine, "x", pair_b)
    half = n_yh // 2
    far_a = lax.ppermute(from_b[:half], "x", pair_a)
    far_b = lax.ppermute(from_a[half:], "x", pair_b)
    own = [mine, from_a, from_b, far_a, far_b]
    other = [lax.ppermute(v, "c", swap) for v in own]
    place = jnp.stack([lax.axis_index("c"), lax.axis_index("x")]).astype(jnp.int32)
    near, far = 3 * each, each
    lanes = 512
    (proj,) = call(
        functools.partial(project_kernel, 3),
        [((3 * hid, near), F32)],
        (place, *own[:3], *other[:3], expert_weights),
        smem=1,
        flops=1 << 31,
    )
    grads, left = call(
        functools.partial(grad_kernel, 3, 2),
        [(expert_weights.shape, BF16), ((3 * hid, lanes), BF16)],
        (place, proj, *own, *other, expert_weights),
        smem=1,
        scratch=[pltpu.VMEM((3 * hid, lanes), F32)],
        flops=1 << 32,
    )
    weight_grads = lax.psum_scatter(grads, "z", scatter_dimension=2, tiled=True).astype(F32)
    shape = (n_yh, n_x, n_yl, BLOCK, width)
    y_own, y_other = call(
        functools.partial(output_kernel, near, far),
        [(shape, BF16), (shape, BF16)],
        (place, left, expert_weights),
        smem=1,
        flops=1 << 32,
    )
    partner = lax.ppermute(y_other, "c", swap)
    y = (y_own.astype(F32) + partner.astype(F32)).astype(BF16)
    home = lax.all_to_all(y.reshape(-1, BLOCK, width), ("yh", "x", "yl"), 0, 0, tiled=True)
    mixed, grad_tokens = call(
        combine_kernel,
        [((n_tok, width), BF16)] * 2,
        (home.reshape(window, n_x * n_yl, BLOCK, width), sel, selw),
        flops=1 << 28,
    )
    return mixed, grad_tokens, weight_grads


def solution(mesh):
    n_ep, n_edp, n_tp = mesh.devices.shape
    side = 4
    fine = Mesh(
        mesh.devices.reshape(side, n_ep // side, n_edp, n_tp // 2, 2), ("yh", "x", "z", "yl", "c")
    )
    group, feat = ("yh", "x", "z"), ("yl", "c")
    hid = ("yh", "x", "yl", "c")
    placed = (P(group, feat), P(group, feat), P(group, None), P(group, None), P(None, hid, None))
    return jax.shard_map(
        shards,
        mesh=fine,
        in_specs=placed,
        out_specs=(P(group, feat), P(group, feat), P(None, hid, "z")),
        check_vma=False,
    )
```
